16 devices in a mesh: fsdp: 16 (over z, y, x, core).
Axes of the slice: x: 2, y: 2, z: 2, core: 2. Of those that a mesh axis runs over, the one named last changes fastest.
Arguments:
- tokens: int32 [16, 2048], P('fsdp')
- positions: int32 [16, 2048], P('fsdp')
- tok_table: float32 [49152, 768], P('fsdp')
- pos_table: float32 [8192, 768], P('fsdp')
- ln1_gain: float32 [768], P('fsdp')
- ln1_bias: float32 [768], P('fsdp')
- w_qkv: float32 [768, 896], P('fsdp')
- b_qkv: float32 [896], P('fsdp')
- w_out: float32 [768, 768], P('fsdp')
- b_out: float32 [768], P('fsdp')
- ln2_gain: float32 [768], P('fsdp')
- ln2_bias: float32 [768], P('fsdp')
- w_fc: float32 [768, 3072], P('fsdp')
- b_fc: float32 [3072], P('fsdp')
- w_proj: float32 [3072, 768], P('fsdp')
- b_proj: float32 [768], P('fsdp')
- grad_out: bfloat16 [16, 2048, 768], P('fsdp')
Outputs:
- output 1: bfloat16 [16, 2048, 768], P('fsdp')
- output 2: float32 [49152, 768], P('fsdp')
- output 3: float32 [8192, 768], P('fsdp')
- output 4: float32 [768], P('fsdp')
- output 5: float32 [768], P('fsdp')
- output 6: float32 [768, 896], P('fsdp')
- output 7: float32 [896], P('fsdp')
- output 8: float32 [768, 768], P('fsdp')
- output 9: float32 [768], P('fsdp')
- output 10: float32 [768], P('fsdp')
- output 11: float32 [768], P('fsdp')
- output 12: float32 [768, 3072], P('fsdp')
- output 13: float32 [3072], P('fsdp')
- output 14: float32 [3072, 768], P('fsdp')
- output 15: float32 [768], P('fsdp')
All inputs are finite; a program needn't handle non-finite values.
Results may differ from the reference program's by a relative error of at most 0.02.
Values are sent between devices in bfloat16 or wider.
A program may use at most 1 GiB of HBM per device.

```python
import jax
import jax.numpy as jnp
from jax import lax

BATCH = 16
SEQ = 2048
D = 768
HEADS = 12
HEAD = 64
FF = 3072
VOCAB = 49152
POS = 8192
DOC_CUTS = 3
QKV = D + 2 * HEAD


def draw_ids(base_key):
    key_u, key_v, key_w, key_cut, key_off = jax.random.split(base_key, 5)
    upper_id = jax.random.randint(key_u, (BATCH, SEQ), 0, VOCAB)
    middle_id = jax.random.randint(key_v, (BATCH, SEQ), 0, upper_id + 1)
    tokens = jax.random.randint(key_w, (BATCH, SEQ), 0, middle_id + 1)
    tokens = tokens.at[0, 0].set(VOCAB - 1).at[1, 0].set(0)
    cut_at = jax.random.randint(key_cut, (BATCH, DOC_CUTS), 1, SEQ)
    column = jnp.arange(SEQ)
    row_ids = jnp.arange(BATCH)
    is_start = jnp.any(cut_at[:, None, :] == column[None, :, None], axis=-1)
    is_start = is_start & (row_ids[:, None] > 0)
    last_start = lax.cummax(jnp.where(is_start, column[None, :], 0), axis=1)
    offset = jax.random.randint(key_off, (BATCH, 1), 0, POS - SEQ + 1)
    offset = offset.at[0, 0].set(POS - SEQ)
    positions = jnp.where(last_start == 0, offset + column[None, :], column[None, :] - last_start)
    return tokens.astype(jnp.int32), positions.astype(jnp.int32)


def setup_inputs(seed: int = 0) -> dict:
    key_list = jax.random.split(jax.random.key(seed), 16)
    tokens, positions = draw_ids(key_list[0])

    def normal(key_index, arr_shape, std_dev):
        return jax.random.normal(key_list[key_index], arr_shape, jnp.float32) * std_dev

    return {
        'tokens': tokens,
        'positions': positions,
        'tok_table': normal(1, (VOCAB, D), 0.7),
        'pos_table': normal(2, (POS, D), 0.7),
        'ln1_gain': 1.0 + normal(3, (D,), 0.2),
        'ln1_bias': normal(4, (D,), 0.2),
        'w_qkv': normal(5, (D, QKV), D ** -0.5),
        'b_qkv': normal(6, (QKV,), 0.3),
        'w_out': normal(7, (D, D), D ** -0.5),
        'b_out': normal(8, (D,), 0.2),
        'ln2_gain': 1.0 + normal(9, (D,), 0.2),
        'ln2_bias': normal(10, (D,), 0.2),
        'w_fc': normal(11, (D, FF), D ** -0.5),
        'b_fc': normal(12, (FF,), 0.3),
        'w_proj': normal(13, (FF, D), FF ** -0.5),
        'b_proj': normal(14, (D,), 0.2),
        'grad_out': normal(15, (BATCH, SEQ, D), 1.0).astype(jnp.bfloat16),
    }


def as_bf16(values):
    return values.astype(jnp.bfloat16).astype(jnp.float32)


def layer_norm(rows_in, ln_gain, ln_shift):
    row_mean = jnp.mean(rows_in, axis=-1, keepdims=True)
    centered = rows_in - row_mean
    row_var = jnp.mean(centered * centered, axis=-1, keepdims=True)
    return centered * lax.rsqrt(row_var + 1e-5) * ln_gain + ln_shift


def layer_fwd(weights, x_seq):
    (ln1_gain, ln1_bias, w_qkv, b_qkv, w_out, b_out, ln2_gain, ln2_bias, w_fc, b_fc, w_proj, b_proj) = weights
    ln1_act = as_bf16(layer_norm(x_seq, ln1_gain, ln1_bias))
    qkv_act = as_bf16(jnp.dot(ln1_act, w_qkv, preferred_element_type=jnp.float32) + b_qkv)
    query_heads = qkv_act[:, :D].reshape(SEQ, HEADS, HEAD)
    key_head = qkv_act[:, D:D + HEAD]
    value_head = qkv_act[:, D + HEAD:]
    scores = jnp.einsum('shd,td->hst', query_heads, key_head) * HEAD ** -0.5
    causal = jnp.arange(SEQ)[:, None] >= jnp.arange(SEQ)[None, :]
    attn_prob = as_bf16(jax.nn.softmax(jnp.where(causal[None], scores, -1e30), axis=-1))
    context = as_bf16(jnp.einsum('hst,td->shd', attn_prob, value_head)).reshape(SEQ, D)
    hidden1 = as_bf16(x_seq + jnp.dot(context, w_out, preferred_element_type=jnp.float32) + b_out)
    ln2_act = as_bf16(layer_norm(hidden1, ln2_gain, ln2_bias))
    pre_fc = as_bf16(jnp.dot(ln2_act, w_fc, preferred_element_type=jnp.float32) + b_fc)
    act_fc = as_bf16(jax.nn.gelu(pre_fc, approximate=True))
    return as_bf16(hidden1 + jnp.dot(act_fc, w_proj, preferred_element_type=jnp.float32) + b_proj)


def reference(tokens, positions, tok_table, pos_table, ln1_gain, ln1_bias, w_qkv, b_qkv, w_out, b_out, ln2_gain, ln2_bias, w_fc, b_fc, w_proj, b_proj, grad_out):
    weights = tuple(as_bf16(master) for master in (ln1_gain, ln1_bias, w_qkv, b_qkv, w_out, b_out, ln2_gain, ln2_bias, w_fc, b_fc, w_proj, b_proj))
    x_all = as_bf16(as_bf16(tok_table[tokens]) + as_bf16(pos_table[positions]))

    def seq_step(grad_acc, seq_pair):
        x_seq, dy_seq = seq_pair
        y_seq, pull_back = jax.vjp(layer_fwd, weights, x_seq)
        d_weights, d_x = pull_back(dy_seq.astype(jnp.float32))
        grad_acc = tuple(acc_sum + seq_grad for acc_sum, seq_grad in zip(grad_acc, d_weights))
        return grad_acc, (y_seq.astype(jnp.bfloat16), d_x)

    zero_acc = tuple(jnp.zeros_like(weight) for weight in weights)
    grad_acc, (hidden_out, d_x0) = lax.scan(seq_step, zero_acc, (x_all, grad_out))
    flat_dx = d_x0.reshape(BATCH * SEQ, D)
    g_tok_table = jax.ops.segment_sum(flat_dx, tokens.reshape(BATCH * SEQ), num_segments=VOCAB)
    g_pos_table = jax.ops.segment_sum(flat_dx, positions.reshape(BATCH * SEQ), num_segments=POS)
    (g_ln1_gain, g_ln1_bias, g_w_qkv, g_b_qkv, g_w_out, g_b_out, g_ln2_gain, g_ln2_bias, g_w_fc, g_b_fc, g_w_proj, g_b_proj) = grad_acc
    return (hidden_out, g_tok_table, g_pos_table, g_ln1_gain, g_ln1_bias, g_w_qkv, g_b_qkv, g_w_out, g_b_out, g_ln2_gain, g_ln2_bias, g_w_fc, g_b_fc, g_w_proj, g_b_proj)
```

```python
import jax
import jax.numpy as jnp
from jax import lax
from jax.experimental import pallas as pl
from jax.experimental.pallas import tpu as pltpu
from jax.sharding import PartitionSpec as P

N_DEV = 16
HEAD = 64
TILE = 256
TOK_SLOTS = 192
POS_SLOTS = 144
BF = jnp.bfloat16
F32 = jnp.float32


def exchange_body(num_split, num_bcast, *refs):
    num = num_split + num_bcast
    srcs, dsts = refs[:num], refs[num:2 * num]
    send_sem, recv_sem, own_sem = refs[2 * num:]
    me = lax.axis_index('fsdp')
    barrier = pltpu.get_barrier_semaphore()
    for off in range(1, N_DEV):
        pl.semaphore_signal(barrier, inc=1, device_id=(lax.rem(me + off, N_DEV),), device_id_type=pl.DeviceIdType.MESH)
    pl.semaphore_wait(barrier, N_DEV - 1)
    copies = []
    for off in range(1, N_DEV):
        peer = lax.rem(me + off, N_DEV)
        for k in range(num):
            copy = pltpu.make_async_remote_copy(
                src_ref=srcs[k].at[peer] if k < num_split else srcs[k],
                dst_ref=dsts[k].at[me],
                send_sem=send_sem.at[k, off],
                recv_sem=recv_sem.at[k, off],
                device_id=(peer,),
                device_id_type=pl.DeviceIdType.MESH,
            )
            copy.start()
            copies.append(copy)
    own = []
    for k in range(num):
        copy = pltpu.make_async_copy(srcs[k].at[me] if k < num_split else srcs[k], dsts[k].at[me], own_sem.at[k])
        copy.start()
        own.append(copy)
    for copy in own:
        copy.wait()
    for copy in copies:
        copy.wait()


def exchange(split, bcast, cid):
    arrays = list(split) + list(bcast)
    num = len(arrays)
    outs = [jax.ShapeDtypeStruct(a.shape, a.dtype) for a in split]
    outs += [jax.ShapeDtypeStruct((N_DEV,) + a.shape, a.dtype) for a in bcast]

    def body(*refs):
        exchange_body(len(split), len(bcast), *refs)

    return pl.pallas_call(
        body,
        out_shape=outs,
        in_specs=[pl.BlockSpec(memory_space=pl.ANY)] * num,
        out_specs=[pl.BlockSpec(memory_space=pl.ANY)] * num,
        scratch_shapes=[
            pltpu.SemaphoreType.DMA((num, N_DEV)),
            pltpu.SemaphoreType.DMA((num, N_DEV)),
            pltpu.SemaphoreType.DMA((num,)),
        ],
        compiler_params=pltpu.CompilerParams(collective_id=cid, has_side_effects=True),
        name=f'exchange_{cid}',
    )(*arrays)


def nt_dot(a, b):
    return lax.dot_general(a, b, (((1,), (1,)), ((), ())), preferred_element_type=F32)


def nn_dot(a, b):
    return lax.dot_general(a, b, (((1,), (0,)), ((), ())), preferred_element_type=F32)


def attn_fwd_tile(qi, q_ref, kv_ref, c_ref, lse_ref, s_ref, p_ref):
    q = q_ref[...] * BF(0.125)
    causal = lax.broadcasted_iota(jnp.int32, (TILE, TILE), 0) >= lax.broadcasted_iota(jnp.int32, (TILE, TILE), 1)
    lse = []
    for head in range(2):
        run_max = None
        for j in range(qi + 1):
            s = nt_dot(q, kv_ref[pl.ds(j * TILE, TILE), pl.ds(head * 128, 128)])
            if j == qi:
                s = jnp.where(causal, s, -1e30)
            s_ref[head, :, pl.ds(j * TILE, TILE)] = s
            part = jnp.maximum(s[:, :128], s[:, 128:])
            run_max = part if run_max is None else jnp.maximum(run_max, part)
        row_max = jnp.max(run_max, axis=1, keepdims=True)
        run_sum = None
        for j in range(qi + 1):
            e = jnp.exp(s_ref[head, :, pl.ds(j * TILE, TILE)] - row_max)
            s_ref[head, :, pl.ds(j * TILE, TILE)] = e
            part = e[:, :128] + e[:, 128:]
            run_sum = part if run_sum is None else run_sum + part
        row_sum = jnp.sum(run_sum, axis=1, keepdims=True)
        inv = 1.0 / row_sum
        for j in range(qi + 1):
            p_ref[head, :, pl.ds(j * TILE, TILE)] = (s_ref[head, :, pl.ds(j * TILE, TILE)] * inv).astype(BF)
        lse.append(row_max + jnp.log(row_sum))
    width = (qi + 1) * TILE
    c = nn_dot(p_ref[0, :, pl.ds(0, width)], kv_ref[pl.ds(0, width), pl.ds(256, 128)])
    c += nn_dot(p_ref[1, :, pl.ds(0, width)], kv_ref[pl.ds(0, width), pl.ds(384, 128)])
    c_ref[...] = c.astype(BF)
    lane = lax.broadcasted_iota(jnp.int32, (TILE, 128), 1)
    both = jnp.where(lane == 0, lse[0], lse[1])
    lse_ref[...] = both.T[:8, :]


def attn_fwd(qkv, kv4):
    seq = qkv.shape[0]
    model = qkv.shape[1] - 2 * HEAD
    pairs, blocks = model // 128, seq // TILE

    def body(*refs):
        for qi in range(blocks):
            @pl.when(pl.program_id(1) == qi)
            def _():
                attn_fwd_tile(qi, *refs)

    return pl.pallas_call(
        body,
        grid=(pairs, blocks),
        in_specs=[
            pl.BlockSpec((TILE, 128), lambda h, i: (i, h)),
            pl.BlockSpec((seq, 512), lambda h, i: (0, 0)),
        ],
        out_specs=[
            pl.BlockSpec((TILE, 128), lambda h, i: (i, h)),
            pl.BlockSpec((8, TILE), lambda h, i: (h, i)),
        ],
        out_shape=[
            jax.ShapeDtypeStruct((seq, model), BF),
            jax.ShapeDtypeStruct((8 * pairs, seq), F32),
        ],
        scratch_shapes=[pltpu.VMEM((2, TILE, seq), F32), pltpu.VMEM((2, TILE, seq), BF)],
        compiler_params=pltpu.CompilerParams(dimension_semantics=('arbitrary', 'arbitrary')),
        cost_estimate=pl.CostEstimate(flops=16 * seq * seq * model // 2, bytes_accessed=8 * seq * model, transcendentals=6 * seq * seq),
        name='attn_fwd',
    )(qkv, kv4)


def attn_bwd_tile(qi, q_ref, dc_ref, lse_ref, kv_ref, kt_ref, dq_ref, p_ref, pb_ref, dp_ref, ds_ref, q2_ref, dc2_ref, dk_acc, dv_acc):
    q = q_ref[...] * BF(0.125)
    dc = dc_ref[...]
    first = (lax.broadcasted_iota(jnp.int32, (1, 128), 1) < HEAD).astype(F32)
    for head in range(2):
        keep = (first if head == 0 else 1.0 - first).astype(BF)
        q2_ref[pl.ds(head * TILE, TILE), :] = q * keep
        dc2_ref[pl.ds(head * TILE, TILE), :] = dc * keep
    causal = lax.broadcasted_iota(jnp.int32, (TILE, TILE), 0) <= lax.broadcasted_iota(jnp.int32, (TILE, TILE), 1)
    width = (qi + 1) * TILE
    dq_parts = []
    for head in range(2):
        cols = pl.ds(head * TILE, TILE)
        lse_row = lse_ref[pl.ds(head, 1), :]
        run = None
        for j in range(qi + 1):
            rows = pl.ds(j * TILE, TILE)
            s = nt_dot(kv_ref[rows, pl.ds(head * 128, 128)], q)
            if j == qi:
                s = jnp.where(causal, s, -1e30)
            p = jnp.exp(s - lse_row)
            p_ref[rows, cols] = p
            pb_ref[rows, cols] = p.astype(BF)
            dp = nt_dot(kv_ref[rows, pl.ds(256 + head * 128, 128)], dc).astype(BF)
            dp_ref[rows, cols] = dp
            part = jnp.sum(p * dp.astype(F32), axis=0, keepdims=True)
            run = part if run is None else run + part
        for j in range(qi + 1):
            rows = pl.ds(j * TILE, TILE)
            ds_ref[rows, cols] = (p_ref[rows, cols] * (dp_ref[rows, cols].astype(F32) - run)).astype(BF)
        dq_parts.append(nn_dot(kt_ref[:, pl.ds(0, width)], ds_ref[pl.ds(0, width), cols]))
    dq_ref[...] = jnp.concatenate(dq_parts, axis=0).T.astype(BF)
    span = pl.ds(0, width)
    dv_acc[span, :] += nn_dot(pb_ref[span, :], dc2_ref[...])
    dk_acc[span, :] += nn_dot(ds_ref[span, :], q2_ref[...])


def attn_bwd(qkv, d_context, lse, kv4, k_t):
    seq = qkv.shape[0]
    model = qkv.shape[1] - 2 * HEAD
    pairs, blocks = model // 128, seq // TILE

    def body(q_ref, dc_ref, lse_ref, kv_ref, kt_ref, dq_ref, dkv_ref, *scratch):
        dk_acc, dv_acc = scratch[-2:]
        pair, block = pl.program_id(0), pl.program_id(1)

        @pl.when((pair == 0) & (block == 0))
        def _():
            dk_acc[...] = jnp.zeros_like(dk_acc)
            dv_acc[...] = jnp.zeros_like(dv_acc)

        for qi in range(blocks):
            @pl.when(block == qi)
            def _():
                attn_bwd_tile(qi, q_ref, dc_ref, lse_ref, kv_ref, kt_ref, dq_ref, *scratch)

        @pl.when((pair == pairs - 1) & (block == blocks - 1))
        def _():
            dk = dk_acc[...]
            dv = dv_acc[...]
            lane = lax.broadcasted_iota(jnp.int32, dk.shape, 1)
            both = jnp.where(lane < HEAD, dk + pltpu.roll(dk, HEAD, 1), dv + pltpu.roll(dv, HEAD, 1))
            dkv_ref[...] = both.astype(BF)

    return pl.pallas_call(
        body,
        grid=(pairs, blocks),
        in_specs=[
            pl.BlockSpec((TILE, 128), lambda h, i: (i, h)),
            pl.BlockSpec((TILE, 128), lambda h, i: (i, h)),
            pl.BlockSpec((8, TILE), lambda h, i: (h, i)),
            pl.BlockSpec((seq, 512), lambda h, i: (0, 0)),
            pl.BlockSpec((HEAD, seq), lambda h, i: (0, 0)),
        ],
        out_specs=[
            pl.BlockSpec((TILE, 128), lambda h, i: (i, h)),
            pl.BlockSpec((seq, 128), lambda h, i: (0, 0)),
        ],
        out_shape=[
            jax.ShapeDtypeStruct((seq, model), BF),
            jax.ShapeDtypeStruct((seq, 128), BF),
        ],
        scratch_shapes=[
            pltpu.VMEM((seq, 2 * TILE), F32),
            pltpu.VMEM((seq, 2 * TILE), BF),
            pltpu.VMEM((seq, 2 * TILE), BF),
            pltpu.VMEM((seq, 2 * TILE), BF),
            pltpu.VMEM((2 * TILE, 128), BF),
            pltpu.VMEM((2 * TILE, 128), BF),
            pltpu.VMEM((seq, 128), F32),
            pltpu.VMEM((seq, 128), F32),
        ],
        compiler_params=pltpu.CompilerParams(dimension_semantics=('arbitrary', 'arbitrary')),
        cost_estimate=pl.CostEstimate(flops=40 * seq * seq * model // 2, bytes_accessed=10 * seq * model, transcendentals=6 * seq * seq),
        name='attn_bwd',
    )(qkv, d_context, lse, kv4, k_t)


def layer_norm(rows_in, ln_gain, ln_shift):
    row_mean = jnp.mean(rows_in, axis=-1, keepdims=True)
    centered = rows_in - row_mean
    row_var = jnp.mean(centered * centered, axis=-1, keepdims=True)
    return centered * lax.rsqrt(row_var + 1e-5) * ln_gain + ln_shift


def gelu_tanh(pre_act):
    return jax.nn.gelu(pre_act, approximate=True)


def tn_dot(a, b):
    return lax.dot_general(a, b, (((0,), (0,)), ((), ())), preferred_element_type=F32)


def layer_pass(x_emb, grad_out, weights):
    (ln1_gain, ln1_bias, w_qkv, b_qkv, w_out, b_out, ln2_gain, ln2_bias, w_fc, b_fc, w_proj, b_proj) = weights
    model = x_emb.shape[1]
    x_res = x_emb.astype(F32)
    ln1_out, pull_ln1 = jax.vjp(layer_norm, x_res, ln1_gain, ln1_bias)
    ln1_act = ln1_out.astype(BF)
    qkv = (nn_dot(ln1_act, w_qkv) + b_qkv).astype(BF)
    key, value = qkv[:, model:model + HEAD], qkv[:, model + HEAD:]
    zero = jnp.zeros_like(key)
    kv4 = jnp.concatenate([key, zero, zero, key, value, zero, zero, value], axis=1)
    k_t = (key * BF(0.125)).T
    context, lse = attn_fwd(qkv, kv4)
    hidden1 = (x_res + nn_dot(context, w_out) + b_out).astype(BF)
    h1_wide = hidden1.astype(F32)
    ln2_out, pull_ln2 = jax.vjp(layer_norm, h1_wide, ln2_gain, ln2_bias)
    ln2_act = ln2_out.astype(BF)
    pre_fc = (nn_dot(ln2_act, w_fc) + b_fc).astype(BF)
    gelu_val, pull_gelu = jax.vjp(gelu_tanh, pre_fc.astype(F32))
    act_fc = gelu_val.astype(BF)
    hidden_out = (h1_wide + nn_dot(act_fc, w_proj) + b_proj).astype(BF)

    dy_wide = grad_out.astype(F32)
    g_b_proj = jnp.sum(dy_wide, axis=0)
    g_w_proj = tn_dot(act_fc, grad_out)
    d_act_fc = nt_dot(grad_out, w_proj).astype(BF)
    d_pre_fc = pull_gelu(d_act_fc.astype(F32))[0].astype(BF)
    g_b_fc = jnp.sum(d_pre_fc, axis=0, dtype=F32)
    g_w_fc = tn_dot(ln2_act, d_pre_fc)
    d_ln2_act = nt_dot(d_pre_fc, w_fc).astype(BF)
    d_h1_norm, g_ln2_gain, g_ln2_bias = pull_ln2(d_ln2_act.astype(F32))
    d_hidden1 = (dy_wide + d_h1_norm).astype(BF)
    g_b_out = jnp.sum(d_hidden1, axis=0, dtype=F32)
    g_w_out = tn_dot(context, d_hidden1)
    d_context = nt_dot(d_hidden1, w_out).astype(BF)
    d_query, d_kv = attn_bwd(qkv, d_context, lse, kv4, k_t)
    d_qkv = jnp.concatenate([d_query, d_kv], axis=1)
    g_b_qkv = jnp.sum(d_qkv, axis=0, dtype=F32)
    g_w_qkv = tn_dot(ln1_act, d_qkv)
    d_ln1_act = nt_dot(d_qkv, w_qkv).astype(BF)
    d_x_norm, g_ln1_gain, g_ln1_bias = pull_ln1(d_ln1_act.astype(F32))
    d_x0 = d_hidden1.astype(F32) + d_x_norm
    vec_grads = (g_ln1_gain, g_ln1_bias, g_b_qkv, g_b_out, g_ln2_gain, g_ln2_bias, g_b_fc, g_b_proj)
    mat_grads = (g_w_qkv, g_w_out, g_w_fc, g_w_proj)
    return hidden_out, d_x0, vec_grads, mat_grads


def slots_of(ids):
    stripe = lax.rem(ids, N_DEV)
    order = jnp.arange(ids.shape[0])
    earlier = (stripe[:, None] == stripe[None, :]) & (order[None, :] < order[:, None])
    return stripe, jnp.sum(earlier.astype(jnp.int32), axis=1)


def round_place(stripe, slot, per_peer, rnd):
    local = slot - rnd * per_peer
    return jnp.where((local >= 0) & (local < per_peer), stripe * per_peer + local, -1)


def requests(place, rows, per_peer):
    total = N_DEV * per_peer
    hit = jnp.arange(total)[:, None] == place[None, :]
    return jnp.max(jnp.where(hit, rows[None, :], -1), axis=1).reshape(N_DEV, per_peer)


def one_hot(row_ids, col_ids):
    return (row_ids[:, None] == col_ids[None, :]).astype(BF)


def solution(mesh):
    vec_spec = P('fsdp')
    mat_spec = P('fsdp', None)
    act_spec = P('fsdp', None, None)
    param_specs = (vec_spec, vec_spec, mat_spec, vec_spec, mat_spec, vec_spec, vec_spec, vec_spec, mat_spec, vec_spec, mat_spec, vec_spec)
    in_specs = (mat_spec, mat_spec, mat_spec, mat_spec) + param_specs + (act_spec,)
    out_specs = (act_spec, mat_spec, mat_spec) + param_specs

    def device_body(tokens, positions, tok_table, pos_table, ln1_gain, ln1_bias, w_qkv, b_qkv, w_out, b_out, ln2_gain, ln2_bias, w_fc, b_fc, w_proj, b_proj, grad_out):
        tokens, positions, grad_out = tokens[0], positions[0], grad_out[0]
        tok_rows, model = tok_table.shape
        pos_rows = pos_table.shape[0]
        tok_sub, pos_sub = tok_rows // N_DEV, pos_rows // N_DEV

        full = [lax.all_gather(w.astype(BF), 'fsdp', axis=0, tiled=True) for w in (w_qkv, w_out, w_fc, w_proj)]

        tok_row = (tokens // tok_rows) * tok_sub + lax.rem(tokens, tok_rows) // N_DEV
        pos_row = (positions // pos_rows) * pos_sub + lax.rem(positions, pos_rows) // N_DEV
        tok_stripe, tok_slot = slots_of(tokens)
        pos_stripe, pos_slot = slots_of(positions)
        my_rounds = jnp.maximum(jnp.max(tok_slot) // TOK_SLOTS, jnp.max(pos_slot) // POS_SLOTS) + 1

        def places(rnd):
            return round_place(tok_stripe, tok_slot, TOK_SLOTS, rnd), round_place(pos_stripe, pos_slot, POS_SLOTS, rnd)

        def request_block(tok_place, pos_place):
            tok_req = requests(tok_place, tok_row, TOK_SLOTS)
            pos_req = requests(pos_place, pos_row, POS_SLOTS)
            rounds = jnp.broadcast_to(my_rounds, (N_DEV, 1))
            flat = jnp.concatenate([tok_req, pos_req, rounds], axis=1)
            return jnp.pad(flat, ((0, 0), (0, 1024 - flat.shape[1]))).reshape(N_DEV, 8, 128)

        def read_block(block):
            flat = block.reshape(N_DEV, 1024)
            tok_req = flat[:, :TOK_SLOTS].reshape(-1)
            pos_req = flat[:, TOK_SLOTS:TOK_SLOTS + POS_SLOTS].reshape(-1)
            return tok_req, pos_req, jnp.max(flat[:, TOK_SLOTS + POS_SLOTS])

        def stripes(table, sub):
            return table.astype(BF).reshape(sub, N_DEV, model).transpose(1, 0, 2)

        shards = (ln1_gain, ln1_bias, b_qkv, b_out, ln2_gain, ln2_bias, b_fc, b_proj)
        sizes = [v.shape[0] for v in shards]
        vec_block = jnp.pad(jnp.concatenate(shards), (0, 1024 - sum(sizes))).reshape(8, 128)
        tok_place, pos_place = places(0)
        tok_stripes, pos_stripes, req_in, vec_all = exchange(
            [stripes(tok_table, tok_sub), stripes(pos_table, pos_sub), request_block(tok_place, pos_place)], [vec_block], 0)
        tok_stripes = tok_stripes.reshape(tok_rows, model)
        pos_stripes = pos_stripes.reshape(pos_rows, model)
        vec_flat = vec_all.reshape(N_DEV, 1024).astype(BF).astype(F32)
        vecs, start = [], 0
        for size in sizes:
            vecs.append(vec_flat[:, start:start + size].reshape(-1))
            start += size

        tok_req0, pos_req0, rounds = read_block(req_in)
        tok_ids, pos_ids = jnp.arange(tok_rows), jnp.arange(pos_rows)
        tok_cols, pos_cols = jnp.arange(N_DEV * TOK_SLOTS), jnp.arange(N_DEV * POS_SLOTS)

        def fetch(tok_req, pos_req, tok_place, pos_place, cid):
            tok_out = nn_dot(one_hot(tok_req, tok_ids), tok_stripes).astype(BF).reshape(N_DEV, TOK_SLOTS, model)
            pos_out = nn_dot(one_hot(pos_req, pos_ids), pos_stripes).astype(BF).reshape(N_DEV, POS_SLOTS, model)
            tok_in, pos_in = exchange([tok_out, pos_out], [], cid)
            x_tok = nn_dot(one_hot(tok_place, tok_cols), tok_in.reshape(-1, model))
            x_pos = nn_dot(one_hot(pos_place, pos_cols), pos_in.reshape(-1, model))
            return x_tok + x_pos

        def more_fetch(state):
            rnd, x_sum = state
            tok_place, pos_place = places(rnd)
            (block,) = exchange([request_block(tok_place, pos_place)], [], 2)
            tok_req, pos_req, _ = read_block(block)
            return rnd + 1, x_sum + fetch(tok_req, pos_req, tok_place, pos_place, 3)

        x_sum = fetch(tok_req0, pos_req0, tok_place, pos_place, 1)
        _, x_sum = lax.while_loop(lambda state: state[0] < rounds, more_fetch, (jnp.int32(1), x_sum))
        x_emb = x_sum.astype(BF)

        weights = (vecs[0], vecs[1], full[0], vecs[2], full[1], vecs[3], vecs[4], vecs[5], full[2], vecs[6], full[3], vecs[7])
        hidden_out, d_x0, vec_grads, mat_grads = layer_pass(x_emb, grad_out, weights)
        d_rows = d_x0.astype(BF)

        vec_out = jnp.concatenate([g.reshape(N_DEV, -1) for g in vec_grads], axis=1)
        vec_out = jnp.pad(vec_out, ((0, 0), (0, 1024 - vec_out.shape[1]))).reshape(N_DEV, 8, 128)

        def give(tok_place, pos_place, extra, cid):
            tok_out = nn_dot(one_hot(tok_cols, tok_place), d_rows).astype(BF).reshape(N_DEV, TOK_SLOTS, model)
            pos_out = nn_dot(one_hot(pos_cols, pos_place), d_rows).astype(BF).reshape(N_DEV, POS_SLOTS, model)
            return exchange([tok_out, pos_out] + extra, [], cid)

        def take(tok_req, pos_req, tok_in, pos_in):
            return (nn_dot(one_hot(tok_ids, tok_req), tok_in.reshape(-1, model)),
                    nn_dot(one_hot(pos_ids, pos_req), pos_in.reshape(-1, model)))

        tok_in, pos_in, vec_in = give(tok_place, pos_place, [vec_out], 4)
        tok_sum, pos_sum = take(tok_req0, pos_req0, tok_in, pos_in)

        def more_give(state):
            rnd, tok_sum, pos_sum = state
            tok_place, pos_place = places(rnd)
            tok_in, pos_in, block = give(tok_place, pos_place, [request_block(tok_place, pos_place)], 5)
            tok_req, pos_req, _ = read_block(block)
            tok_add, pos_add = take(tok_req, pos_req, tok_in, pos_in)
            return rnd + 1, tok_sum + tok_add, pos_sum + pos_add

        _, tok_sum, pos_sum = lax.while_loop(lambda state: state[0] < rounds, more_give, (jnp.int32(1), tok_sum, pos_sum))
        tok_back, pos_back = exchange(
            [tok_sum.astype(BF).reshape(N_DEV, tok_sub, model), pos_sum.astype(BF).reshape(N_DEV, pos_sub, model)], [], 6)
        g_tok = tok_back.transpose(1, 0, 2).reshape(tok_rows, model).astype(F32)
        g_pos = pos_back.transpose(1, 0, 2).reshape(pos_rows, model).astype(F32)

        vec_sum = jnp.sum(vec_in.reshape(N_DEV, 1024), axis=0)
        g_vecs, start = [], 0
        for size in sizes:
            g_vecs.append(vec_sum[start:start + size])
            start += size
        g_mats = [lax.psum_scatter(g, 'fsdp', scatter_dimension=0, tiled=True) for g in mat_grads]
        return (hidden_out[None], g_tok, g_pos, g_vecs[0], g_vecs[1], g_mats[0], g_vecs[2], g_mats[1], g_vecs[3],
                g_vecs[4], g_vecs[5], g_mats[2], g_vecs[6], g_mats[3], g_vecs[7])

    return jax.shard_map(device_body, mesh=mesh, in_specs=in_specs, out_specs=out_specs, check_vma=False)
```

```python
import jax
import jax.numpy as jnp
from jax import lax
from jax.experimental import pallas as pl
from jax.experimental.layout import Layout, with_layout_constraint
from jax.experimental.pallas import tpu as pltpu
from jax.sharding import PartitionSpec as P

N_DEV = 16
HEAD = 64
TILE = 256
TOK_SLOTS = 192
POS_SLOTS = 144
BF = jnp.bfloat16
F32 = jnp.float32


def exchange_body(num_split, num_bcast, *refs):
    num = num_split + num_bcast
    srcs, dsts = refs[:num], refs[num:2 * num]
    send_sem, recv_sem, own_sem = refs[2 * num:]
    me = lax.axis_index('fsdp')
    barrier = pltpu.get_barrier_semaphore()
    for off in range(1, N_DEV):
        pl.semaphore_signal(barrier, inc=1, device_id=(lax.rem(me + off, N_DEV),), device_id_type=pl.DeviceIdType.MESH)
    pl.semaphore_wait(barrier, N_DEV - 1)
    copies = []
    for off in range(1, N_DEV):
        peer = lax.rem(me + off, N_DEV)
        for k in range(num):
            copy = pltpu.make_async_remote_copy(
                src_ref=srcs[k].at[peer] if k < num_split else srcs[k],
                dst_ref=dsts[k].at[me],
                send_sem=send_sem.at[k, off],
                recv_sem=recv_sem.at[k, off],
                device_id=(peer,),
                device_id_type=pl.DeviceIdType.MESH,
            )
            copy.start()
            copies.append(copy)
    own = []
    for k in range(num):
        copy = pltpu.make_async_copy(srcs[k].at[me] if k < num_split else srcs[k], dsts[k].at[me], own_sem.at[k])
        copy.start()
        own.append(copy)
    for copy in own:
        copy.wait()
    for copy in copies:
        copy.wait()


def exchange(split, bcast, cid):
    arrays = list(split) + list(bcast)
    num = len(arrays)
    outs = [jax.ShapeDtypeStruct(a.shape, a.dtype) for a in split]
    outs += [jax.ShapeDtypeStruct((N_DEV,) + a.shape, a.dtype) for a in bcast]

    def body(*refs):
        exchange_body(len(split), len(bcast), *refs)

    return pl.pallas_call(
        body,
        out_shape=outs,
        in_specs=[pl.BlockSpec(memory_space=pl.ANY)] * num,
        out_specs=[pl.BlockSpec(memory_space=pl.ANY)] * num,
        scratch_shapes=[
            pltpu.SemaphoreType.DMA((num, N_DEV)),
            pltpu.SemaphoreType.DMA((num, N_DEV)),
            pltpu.SemaphoreType.DMA((num,)),
        ],
        compiler_params=pltpu.CompilerParams(collective_id=cid, has_side_effects=True),
        name=f'exchange_{cid}',
    )(*arrays)


def nt_dot(a, b):
    return lax.dot_general(a, b, (((1,), (1,)), ((), ())), preferred_element_type=F32)


def nn_dot(a, b):
    return lax.dot_general(a, b, (((1,), (0,)), ((), ())), preferred_element_type=F32)


def attn_fwd_tile(qi, q_ref, kv_ref, c_ref, lse_ref, s_ref, p_ref):
    q = q_ref[...] * BF(0.125)
    causal = lax.broadcasted_iota(jnp.int32, (TILE, TILE), 0) >= lax.broadcasted_iota(jnp.int32, (TILE, TILE), 1)
    lse = []
    for head in range(2):
        run_max = None
        for j in range(qi + 1):
            s = nt_dot(q, kv_ref[pl.ds(j * TILE, TILE), pl.ds(head * 128, 128)])
            if j == qi:
                s = jnp.where(causal, s, -1e30)
            s_ref[head, :, pl.ds(j * TILE, TILE)] = s
            part = jnp.maximum(s[:, :128], s[:, 128:])
            run_max = part if run_max is None else jnp.maximum(run_max, part)
        row_max = jnp.max(run_max, axis=1, keepdims=True)
        run_sum = None
        for j in range(qi + 1):
            e = jnp.exp(s_ref[head, :, pl.ds(j * TILE, TILE)] - row_max)
            s_ref[head, :, pl.ds(j * TILE, TILE)] = e
            part = e[:, :128] + e[:, 128:]
            run_sum = part if run_sum is None else run_sum + part
        row_sum = jnp.sum(run_sum, axis=1, keepdims=True)
        inv = 1.0 / row_sum
        for j in range(qi + 1):
            p_ref[head, :, pl.ds(j * TILE, TILE)] = (s_ref[head, :, pl.ds(j * TILE, TILE)] * inv).astype(BF)
        lse.append(row_max + jnp.log(row_sum))
    width = (qi + 1) * TILE
    c = nn_dot(p_ref[0, :, pl.ds(0, width)], kv_ref[pl.ds(0, width), pl.ds(256, 128)])
    c += nn_dot(p_ref[1, :, pl.ds(0, width)], kv_ref[pl.ds(0, width), pl.ds(384, 128)])
    c_ref[...] = c.astype(BF)
    lane = lax.broadcasted_iota(jnp.int32, (TILE, 128), 1)
    both = jnp.where(lane == 0, lse[0], lse[1])
    lse_ref[...] = both.T[:8, :]


def attn_fwd(qkv, kv4):
    seq = qkv.shape[0]
    model = qkv.shape[1] - 2 * HEAD
    pairs, blocks = model // 128, seq // TILE

    def body(*refs):
        for qi in range(blocks):
            @pl.when(pl.program_id(1) == qi)
            def _():
                attn_fwd_tile(qi, *refs)

    return pl.pallas_call(
        body,
        grid=(pairs, blocks),
        in_specs=[
            pl.BlockSpec((TILE, 128), lambda h, i: (i, h)),
            pl.BlockSpec((seq, 512), lambda h, i: (0, 0)),
        ],
        out_specs=[
            pl.BlockSpec((TILE, 128), lambda h, i: (i, h)),
            pl.BlockSpec((8, TILE), lambda h, i: (h, i)),
        ],
        out_shape=[
            jax.ShapeDtypeStruct((seq, model), BF),
            jax.ShapeDtypeStruct((8 * pairs, seq), F32),
        ],
        scratch_shapes=[pltpu.VMEM((2, TILE, seq), F32), pltpu.VMEM((2, TILE, seq), BF)],
        compiler_params=pltpu.CompilerParams(dimension_semantics=('arbitrary', 'arbitrary')),
        cost_estimate=pl.CostEstimate(flops=16 * seq * seq * model // 2, bytes_accessed=8 * seq * model, transcendentals=6 * seq * seq),
        name='attn_fwd',
    )(qkv, kv4)


def attn_bwd_tile(qi, q_ref, dc_ref, lse_ref, kv_ref, kt_ref, dq_ref, p_ref, pb_ref, dp_ref, ds_ref, q2_ref, dc2_ref, dk_acc, dv_acc):
    q = q_ref[...] * BF(0.125)
    dc = dc_ref[...]
    first = (lax.broadcasted_iota(jnp.int32, (1, 128), 1) < HEAD).astype(F32)
    for head in range(2):
        keep = (first if head == 0 else 1.0 - first).astype(BF)
        q2_ref[pl.ds(head * TILE, TILE), :] = q * keep
        dc2_ref[pl.ds(head * TILE, TILE), :] = dc * keep
    causal = lax.broadcasted_iota(jnp.int32, (TILE, TILE), 0) <= lax.broadcasted_iota(jnp.int32, (TILE, TILE), 1)
    width = (qi + 1) * TILE
    dq_parts = []
    for head in range(2):
        cols = pl.ds(head * TILE, TILE)
        lse_row = lse_ref[pl.ds(head, 1), :]
        run = None
        for j in range(qi + 1):
            rows = pl.ds(j * TILE, TILE)
            s = nt_dot(kv_ref[rows, pl.ds(head * 128, 128)], q)
            if j == qi:
                s = jnp.where(causal, s, -1e30)
            p = jnp.exp(s - lse_row)
            p_ref[rows, cols] = p
            pb_ref[rows, cols] = p.astype(BF)
            dp = nt_dot(kv_ref[rows, pl.ds(256 + head * 128, 128)], dc).astype(BF)
            dp_ref[rows, cols] = dp
            part = jnp.sum(p * dp.astype(F32), axis=0, keepdims=True)
            run = part if run is None else run + part
        for j in range(qi + 1):
            rows = pl.ds(j * TILE, TILE)
            ds_ref[rows, cols] = (p_ref[rows, cols] * (dp_ref[rows, cols].astype(F32) - run)).astype(BF)
        dq_parts.append(nn_dot(kt_ref[:, pl.ds(0, width)], ds_ref[pl.ds(0, width), cols]))
    dq_ref[...] = jnp.concatenate(dq_parts, axis=0).T.astype(BF)
    span = pl.ds(0, width)
    dv_acc[span, :] += nn_dot(pb_ref[span, :], dc2_ref[...])
    dk_acc[span, :] += nn_dot(ds_ref[span, :], q2_ref[...])


def attn_bwd(qkv, d_context, lse, kv4, k_t):
    seq = qkv.shape[0]
    model = qkv.shape[1] - 2 * HEAD
    pairs, blocks = model // 128, seq // TILE

    def body(q_ref, dc_ref, lse_ref, kv_ref, kt_ref, dq_ref, dkv_ref, *scratch):
        dk_acc, dv_acc = scratch[-2:]
        pair, block = pl.program_id(0), pl.program_id(1)

        @pl.when((pair == 0) & (block == 0))
        def _():
            dk_acc[...] = jnp.zeros_like(dk_acc)
            dv_acc[...] = jnp.zeros_like(dv_acc)

        for qi in range(blocks):
            @pl.when(block == qi)
            def _():
                attn_bwd_tile(qi, q_ref, dc_ref, lse_ref, kv_ref, kt_ref, dq_ref, *scratch)

        @pl.when((pair == pairs - 1) & (block == blocks - 1))
        def _():
            dk = dk_acc[...]
            dv = dv_acc[...]
            lane = lax.broadcasted_iota(jnp.int32, dk.shape, 1)
            both = jnp.where(lane < HEAD, dk + pltpu.roll(dk, HEAD, 1), dv + pltpu.roll(dv, HEAD, 1))
            dkv_ref[...] = both.astype(BF)

    return pl.pallas_call(
        body,
        grid=(pairs, blocks),
        in_specs=[
            pl.BlockSpec((TILE, 128), lambda h, i: (i, h)),
            pl.BlockSpec((TILE, 128), lambda h, i: (i, h)),
            pl.BlockSpec((8, TILE), lambda h, i: (h, i)),
            pl.BlockSpec((seq, 512), lambda h, i: (0, 0)),
            pl.BlockSpec((HEAD, seq), lambda h, i: (0, 0)),
        ],
        out_specs=[
            pl.BlockSpec((TILE, 128), lambda h, i: (i, h)),
            pl.BlockSpec((seq, 128), lambda h, i: (0, 0)),
        ],
        out_shape=[
            jax.ShapeDtypeStruct((seq, model), BF),
            jax.ShapeDtypeStruct((seq, 128), BF),
        ],
        scratch_shapes=[
            pltpu.VMEM((seq, 2 * TILE), F32),
            pltpu.VMEM((seq, 2 * TILE), BF),
            pltpu.VMEM((seq, 2 * TILE), BF),
            pltpu.VMEM((seq, 2 * TILE), BF),
            pltpu.VMEM((2 * TILE, 128), BF),
            pltpu.VMEM((2 * TILE, 128), BF),
            pltpu.VMEM((seq, 128), F32),
            pltpu.VMEM((seq, 128), F32),
        ],
        compiler_params=pltpu.CompilerParams(dimension_semantics=('arbitrary', 'arbitrary')),
        cost_estimate=pl.CostEstimate(flops=40 * seq * seq * model // 2, bytes_accessed=10 * seq * model, transcendentals=6 * seq * seq),
        name='attn_bwd',
    )(qkv, d_context, lse, kv4, k_t)


def layer_norm(rows_in, ln_gain, ln_shift):
    row_mean = jnp.mean(rows_in, axis=-1, keepdims=True)
    centered = rows_in - row_mean
    row_var = jnp.mean(centered * centered, axis=-1, keepdims=True)
    return centered * lax.rsqrt(row_var + 1e-5) * ln_gain + ln_shift


def gelu_tanh(pre_act):
    return jax.nn.gelu(pre_act, approximate=True)


def row_major(a):
    return with_layout_constraint(a, Layout(major_to_minor=tuple(range(a.ndim))))


def tn_dot(a, b):
    return lax.dot_general(a, b, (((0,), (0,)), ((), ())), preferred_element_type=F32)


def layer_pass(x_emb, grad_out, weights):
    (ln1_gain, ln1_bias, w_qkv, b_qkv, w_out, b_out, ln2_gain, ln2_bias, w_fc, b_fc, w_proj, b_proj) = weights
    model = x_emb.shape[1]
    x_res = x_emb.astype(F32)
    ln1_out, pull_ln1 = jax.vjp(layer_norm, x_res, ln1_gain, ln1_bias)
    ln1_act = ln1_out.astype(BF)
    qkv = row_major((nn_dot(ln1_act, w_qkv) + b_qkv).astype(BF))
    key, value = qkv[:, model:model + HEAD], qkv[:, model + HEAD:]
    zero = jnp.zeros_like(key)
    kv4 = jnp.concatenate([key, zero, zero, key, value, zero, zero, value], axis=1)
    k_t = (key * BF(0.125)).T
    context, lse = attn_fwd(qkv, kv4)
    hidden1 = (x_res + nn_dot(context, w_out) + b_out).astype(BF)
    h1_wide = hidden1.astype(F32)
    ln2_out, pull_ln2 = jax.vjp(layer_norm, h1_wide, ln2_gain, ln2_bias)
    ln2_act = ln2_out.astype(BF)
    pre_fc = (nn_dot(ln2_act, w_fc) + b_fc).astype(BF)
    gelu_val, pull_gelu = jax.vjp(gelu_tanh, pre_fc.astype(F32))
    act_fc = gelu_val.astype(BF)
    hidden_out = (h1_wide + nn_dot(act_fc, w_proj) + b_proj).astype(BF)

    dy_wide = grad_out.astype(F32)
    g_b_proj = jnp.sum(dy_wide, axis=0)
    g_w_proj = tn_dot(act_fc, grad_out)
    d_act_fc = nt_dot(grad_out, w_proj).astype(BF)
    d_pre_fc = pull_gelu(d_act_fc.astype(F32))[0].astype(BF)
    g_b_fc = jnp.sum(d_pre_fc, axis=0, dtype=F32)
    g_w_fc = tn_dot(ln2_act, d_pre_fc)
    d_ln2_act = nt_dot(d_pre_fc, w_fc).astype(BF)
    d_h1_norm, g_ln2_gain, g_ln2_bias = pull_ln2(d_ln2_act.astype(F32))
    d_hidden1 = (dy_wide + d_h1_norm).astype(BF)
    g_b_out = jnp.sum(d_hidden1, axis=0, dtype=F32)
    g_w_out = tn_dot(context, d_hidden1)
    d_context = row_major(nt_dot(d_hidden1, w_out).astype(BF))
    d_context, g_w_out, g_w_fc, g_w_proj = lax.optimization_barrier((d_context, g_w_out, g_w_fc, g_w_proj))
    d_query, d_kv = attn_bwd(qkv, d_context, lse, kv4, k_t)
    d_qkv = jnp.concatenate([d_query, d_kv], axis=1)
    g_b_qkv = jnp.sum(d_qkv, axis=0, dtype=F32)
    g_w_qkv = tn_dot(ln1_act, d_qkv)
    d_ln1_act = nt_dot(d_qkv, w_qkv).astype(BF)
    d_x_norm, g_ln1_gain, g_ln1_bias = pull_ln1(d_ln1_act.astype(F32))
    d_x0 = d_hidden1.astype(F32) + d_x_norm
    vec_grads = (g_ln1_gain, g_ln1_bias, g_b_qkv, g_b_out, g_ln2_gain, g_ln2_bias, g_b_fc, g_b_proj)
    mat_grads = (g_w_qkv, g_w_out, g_w_fc, g_w_proj)
    return hidden_out, d_x0, vec_grads, mat_grads


def slots_of(ids):
    stripe = lax.rem(ids, N_DEV)
    order = jnp.arange(ids.shape[0])
    earlier = (stripe[:, None] == stripe[None, :]) & (order[None, :] < order[:, None])
    return stripe, jnp.sum(earlier.astype(jnp.int32), axis=1)


def round_place(stripe, slot, per_peer, rnd):
    local = slot - rnd * per_peer
    return jnp.where((local >= 0) & (local < per_peer), stripe * per_peer + local, -1)


def requests(place, rows, per_peer):
    total = N_DEV * per_peer
    hit = jnp.arange(total)[:, None] == place[None, :]
    return jnp.max(jnp.where(hit, rows[None, :], -1), axis=1).reshape(N_DEV, per_peer)


def one_hot(row_ids, col_ids):
    return (row_ids[:, None] == col_ids[None, :]).astype(BF)


def solution(mesh):
    vec_spec = P('fsdp')
    mat_spec = P('fsdp', None)
    act_spec = P('fsdp', None, None)
    param_specs = (vec_spec, vec_spec, mat_spec, vec_spec, mat_spec, vec_spec, vec_spec, vec_spec, mat_spec, vec_spec, mat_spec, vec_spec)
    in_specs = (mat_spec, mat_spec, mat_spec, mat_spec) + param_specs + (act_spec,)
    out_specs = (act_spec, mat_spec, mat_spec) + param_specs

    def device_body(tokens, positions, tok_table, pos_table, ln1_gain, ln1_bias, w_qkv, b_qkv, w_out, b_out, ln2_gain, ln2_bias, w_fc, b_fc, w_proj, b_proj, grad_out):
        tokens, positions, grad_out = tokens[0], positions[0], grad_out[0]
        tok_rows, model = tok_table.shape
        pos_rows = pos_table.shape[0]
        tok_sub, pos_sub = tok_rows // N_DEV, pos_rows // N_DEV

        pos_full = lax.all_gather(pos_table.astype(BF), 'fsdp', axis=0, tiled=True)
        qkv_full = lax.all_gather(w_qkv.astype(BF), 'fsdp', axis=0, tiled=True)

        tok_row = lax.div(tokens, tok_rows) * tok_sub + lax.div(lax.rem(tokens, tok_rows), N_DEV)
        pos_row = lax.div(positions, pos_rows) * pos_sub + lax.div(lax.rem(positions, pos_rows), N_DEV)
        tok_stripe, tok_slot = slots_of(tokens)
        pos_stripe, pos_slot = slots_of(positions)
        my_rounds = jnp.maximum(lax.div(jnp.max(tok_slot), TOK_SLOTS), lax.div(jnp.max(pos_slot), POS_SLOTS)) + 1

        def places(rnd):
            return round_place(tok_stripe, tok_slot, TOK_SLOTS, rnd), round_place(pos_stripe, pos_slot, POS_SLOTS, rnd)

        def request_block(tok_place, pos_place):
            tok_req = requests(tok_place, tok_row, TOK_SLOTS)
            pos_req = requests(pos_place, pos_row, POS_SLOTS)
            rounds = jnp.broadcast_to(my_rounds, (N_DEV, 1))
            flat = jnp.concatenate([tok_req, pos_req, rounds], axis=1)
            return jnp.pad(flat, ((0, 0), (0, 1024 - flat.shape[1]))).reshape(N_DEV, 8, 128)

        def read_block(block):
            flat = block.reshape(N_DEV, 1024)
            tok_req = flat[:, :TOK_SLOTS].reshape(-1)
            pos_req = flat[:, TOK_SLOTS:TOK_SLOTS + POS_SLOTS].reshape(-1)
            return tok_req, pos_req, jnp.max(flat[:, TOK_SLOTS + POS_SLOTS])

        def stripes(table, sub):
            return table.astype(BF).reshape(sub, N_DEV, model).transpose(1, 0, 2)

        shards = (ln1_gain, ln1_bias, b_qkv, b_out, ln2_gain, ln2_bias, b_fc, b_proj)
        sizes = [v.shape[0] for v in shards]
        vec_block = jnp.pad(jnp.concatenate(shards), (0, 1024 - sum(sizes))).reshape(8, 128)
        tok_place, pos_place = places(0)
        tok_stripes, req_in, vec_all = exchange([stripes(tok_table, tok_sub), request_block(tok_place, pos_place)], [vec_block], 0)
        tok_stripes = tok_stripes.reshape(tok_rows, model)
        vec_flat = vec_all.reshape(N_DEV, 1024).astype(BF).astype(F32)
        vecs, start = [], 0
        for size in sizes:
            vecs.append(vec_flat[:, start:start + size].reshape(-1))
            start += size

        tok_req0, pos_req0, rounds = read_block(req_in)
        tok_ids, pos_ids = jnp.arange(tok_rows), jnp.arange(pos_rows)
        tok_cols, pos_cols = jnp.arange(N_DEV * TOK_SLOTS), jnp.arange(N_DEV * POS_SLOTS)

        def fetch(tok_req, tok_place, cid):
            tok_out = nn_dot(one_hot(tok_req, tok_ids), tok_stripes).astype(BF).reshape(N_DEV, TOK_SLOTS, model)
            (tok_in,) = exchange([tok_out], [], cid)
            return nn_dot(one_hot(tok_place, tok_cols), tok_in.reshape(-1, model))

        def slow_fetch():
            def step(state):
                rnd, x_sum = state
                tok_place, pos_place = places(rnd)
                (block,) = exchange([request_block(tok_place, pos_place)], [], 2)
                return rnd + 1, x_sum + fetch(read_block(block)[0], tok_place, 3)

            _, x_sum = lax.while_loop(lambda state: state[0] < rounds, step, (jnp.int32(0), jnp.zeros((tokens.shape[0], model), F32)))
            return x_sum.astype(BF)

        x_tok = fetch(tok_req0, tok_place, 1).astype(BF)
        x_tok = lax.cond(rounds > 1, slow_fetch, lambda: x_tok)
        x_pos = jnp.take(pos_full, positions, axis=0)
        x_emb = (x_tok.astype(F32) + x_pos.astype(F32)).astype(BF)
        x_emb, late = lax.optimization_barrier((x_emb, (w_out.astype(BF), w_fc.astype(BF), w_proj.astype(BF))))
        full = [qkv_full] + [lax.all_gather(w, 'fsdp', axis=0, tiled=True) for w in late]

        weights = (vecs[0], vecs[1], full[0], vecs[2], full[1], vecs[3], vecs[4], vecs[5], full[2], vecs[6], full[3], vecs[7])
        hidden_out, d_x0, vec_grads, mat_grads = layer_pass(x_emb, grad_out, weights)
        d_rows = d_x0.astype(BF)

        def scatter_sum(grad):
            return lax.psum_scatter(grad, 'fsdp', scatter_dimension=0, tiled=True)

        early = [scatter_sum(g) for g in mat_grads[2:]]
        d_rows, early, late_grads = lax.optimization_barrier((d_rows, early, mat_grads[:2]))
        g_mats = [scatter_sum(g) for g in late_grads] + list(early)

        vec_out = jnp.concatenate([g.reshape(N_DEV, -1) for g in vec_grads], axis=1)
        vec_out = jnp.pad(vec_out, ((0, 0), (0, 1024 - vec_out.shape[1]))).reshape(N_DEV, 8, 128)

        def give(tok_place, pos_place, extra, cid):
            tok_out = nn_dot(one_hot(tok_cols, tok_place), d_rows).astype(BF).reshape(N_DEV, TOK_SLOTS, model)
            pos_out = nn_dot(one_hot(pos_cols, pos_place), d_rows).astype(BF).reshape(N_DEV, POS_SLOTS, model)
            return exchange([tok_out, pos_out] + extra, [], cid)

        def take(tok_req, pos_req, tok_in, pos_in):
            return (nn_dot(one_hot(tok_ids, tok_req), tok_in.reshape(-1, model)),
                    nn_dot(one_hot(pos_ids, pos_req), pos_in.reshape(-1, model)))

        tok_in, pos_in, vec_in = give(tok_place, pos_place, [vec_out], 4)
        tok_sum, pos_sum = take(tok_req0, pos_req0, tok_in, pos_in)
        tok_sum, pos_sum = tok_sum.astype(BF), pos_sum.astype(BF)

        def slow_give():
            def step(state):
                rnd, tok_sum, pos_sum = state
                tok_place, pos_place = places(rnd)
                tok_in, pos_in, block = give(tok_place, pos_place, [request_block(tok_place, pos_place)], 5)
                tok_req, pos_req, _ = read_block(block)
                tok_add, pos_add = take(tok_req, pos_req, tok_in, pos_in)
                return rnd + 1, tok_sum + tok_add, pos_sum + pos_add

            zeros = (jnp.zeros((tok_rows, model), F32), jnp.zeros((pos_rows, model), F32))
            _, tok_sum, pos_sum = lax.while_loop(lambda state: state[0] < rounds, step, (jnp.int32(0),) + zeros)
            return tok_sum.astype(BF), pos_sum.astype(BF)

        tok_sum, pos_sum = lax.cond(rounds > 1, slow_give, lambda: (tok_sum, pos_sum))
        tok_back, pos_back = exchange([tok_sum.reshape(N_DEV, tok_sub, model), pos_sum.reshape(N_DEV, pos_sub, model)], [], 6)
        g_tok = tok_back.transpose(1, 0, 2).reshape(tok_rows, model).astype(F32)
        g_pos = pos_back.transpose(1, 0, 2).reshape(pos_rows, model).astype(F32)

        vec_sum = jnp.sum(vec_in.reshape(N_DEV, 1024), axis=0)
        g_vecs, start = [], 0
        for size in sizes:
            g_vecs.append(vec_sum[start:start + size])
            start += size
        return (hidden_out[None], g_tok, g_pos, g_vecs[0], g_vecs[1], g_mats[0], g_vecs[2], g_mats[1], g_vecs[3],
                g_vecs[4], g_vecs[5], g_mats[2], g_vecs[6], g_mats[3], g_vecs[7])

    return jax.shard_map(device_body, mesh=mesh, in_specs=in_specs, out_specs=out_specs, check_vma=False)
```

```python
import jax
import jax.numpy as jnp
from jax import lax
from jax.experimental import pallas as pl
from jax.experimental.layout import Layout, with_layout_constraint
from jax.experimental.pallas import tpu as pltpu
from jax.sharding import PartitionSpec as P

N_DEV = 16
HEAD = 64
TILE = 256
GROUP = 4
TOK_SLOTS = 192
POS_SLOTS = 144
BF = jnp.bfloat16
F32 = jnp.float32


def exchange_body(num_split, num_bcast, *refs):
    num = num_split + num_bcast
    srcs, dsts = refs[:num], refs[num:2 * num]
    send_sem, recv_sem, own_sem = refs[2 * num:]
    me = lax.axis_index('fsdp')
    barrier = pltpu.get_barrier_semaphore()
    for off in range(1, N_DEV):
        pl.semaphore_signal(barrier, inc=1, device_id=(lax.rem(me + off, N_DEV),), device_id_type=pl.DeviceIdType.MESH)
    pl.semaphore_wait(barrier, N_DEV - 1)
    copies = []
    for off in range(1, N_DEV):
        peer = lax.rem(me + off, N_DEV)
        for k in range(num):
            copy = pltpu.make_async_remote_copy(
                src_ref=srcs[k].at[peer] if k < num_split else srcs[k],
                dst_ref=dsts[k].at[me],
                send_sem=send_sem.at[k, off],
                recv_sem=recv_sem.at[k, off],
                device_id=(peer,),
                device_id_type=pl.DeviceIdType.MESH,
            )
            copy.start()
            copies.append(copy)
    own = []
    for k in range(num):
        copy = pltpu.make_async_copy(srcs[k].at[me] if k < num_split else srcs[k], dsts[k].at[me], own_sem.at[k])
        copy.start()
        own.append(copy)
    for copy in own:
        copy.wait()
    for copy in copies:
        copy.wait()


def exchange(split, bcast, cid):
    arrays = list(split) + list(bcast)
    num = len(arrays)
    outs = [jax.ShapeDtypeStruct(a.shape, a.dtype) for a in split]
    outs += [jax.ShapeDtypeStruct((N_DEV,) + a.shape, a.dtype) for a in bcast]

    def body(*refs):
        exchange_body(len(split), len(bcast), *refs)

    return pl.pallas_call(
        body,
        out_shape=outs,
        in_specs=[pl.BlockSpec(memory_space=pl.ANY)] * num,
        out_specs=[pl.BlockSpec(memory_space=pl.ANY)] * num,
        scratch_shapes=[
            pltpu.SemaphoreType.DMA((num, N_DEV)),
            pltpu.SemaphoreType.DMA((num, N_DEV)),
            pltpu.SemaphoreType.DMA((num,)),
        ],
        compiler_params=pltpu.CompilerParams(collective_id=cid, has_side_effects=True),
        name=f'exchange_{cid}',
    )(*arrays)


def enter_all(me):
    barrier = pltpu.get_barrier_semaphore()
    for off in range(1, N_DEV):
        pl.semaphore_signal(barrier, inc=1, device_id=(lax.rem(me + off, N_DEV),), device_id_type=pl.DeviceIdType.MESH)
    pl.semaphore_wait(barrier, N_DEV - 1)


def iota(shape, axis):
    return lax.broadcasted_iota(jnp.int32, shape, axis)


def fetch_body(req_ref, place_ref, table_ref, x_ref, send_buf, recv_buf, acc_ref, send_sem, recv_sem):
    me = lax.axis_index('fsdp')
    rows = table_ref.shape[0]
    seq, model = x_ref.shape
    enter_all(me)

    def remote(off):
        return pltpu.make_async_remote_copy(
            src_ref=send_buf.at[off], dst_ref=recv_buf.at[off], send_sem=send_sem.at[off], recv_sem=recv_sem.at[off],
            device_id=(lax.rem(me + off, N_DEV),), device_id_type=pl.DeviceIdType.MESH)

    def answer(off):
        pick = (req_ref[lax.rem(me + off, N_DEV)] == iota((TOK_SLOTS, rows), 1)).astype(F32).astype(BF)
        return nn_dot(pick, table_ref[...]).astype(BF)

    def produce(off, carry):
        send_buf[off] = answer(off)

        @pl.when(off >= 2)
        def _():
            remote(off - 1).start()
        return carry

    lax.fori_loop(1, N_DEV, produce, 0)
    recv_buf[0] = answer(0)
    remote(N_DEV - 1).start()

    wide = GROUP * TOK_SLOTS
    lane = iota((1, wide), 1)
    part = sum((lane >= k * TOK_SLOTS).astype(jnp.int32) for k in range(1, GROUP))
    for g in range(N_DEV // GROUP):
        for off in range(g * GROUP, (g + 1) * GROUP):
            if off:
                remote(off).wait_recv()
        source = lax.rem(me + N_DEV - g * GROUP - part, N_DEV)
        target = source * TOK_SLOTS + lane - part * TOK_SLOTS
        block = recv_buf[pl.ds(g * GROUP, GROUP)].reshape(wide, model)

        def place(r, carry):
            span = pl.ds(r * TILE, TILE)
            pick = (place_ref[span, :] == target).astype(F32).astype(BF)
            add = nn_dot(pick, block)
            if g == 0:
                acc_ref[span, :] = add
            elif g < N_DEV // GROUP - 1:
                acc_ref[span, :] += add
            else:
                x_ref[span, :] = (acc_ref[span, :] + add).astype(BF)
            return carry

        lax.fori_loop(0, seq // TILE, place, 0)
    for off in range(1, N_DEV):
        remote(off).wait_send()


def fetch_rows(tok_req, tok_place, table, cid):
    seq, model = tok_place.shape[0], table.shape[1]
    return pl.pallas_call(
        fetch_body,
        out_shape=jax.ShapeDtypeStruct((seq, model), BF),
        in_specs=[pl.BlockSpec(memory_space=pltpu.VMEM)] * 3,
        out_specs=pl.BlockSpec(memory_space=pltpu.VMEM),
        scratch_shapes=[
            pltpu.VMEM((N_DEV, TOK_SLOTS, model), BF),
            pltpu.VMEM((N_DEV, TOK_SLOTS, model), BF),
            pltpu.VMEM((seq, model), F32),
            pltpu.SemaphoreType.DMA((N_DEV,)),
            pltpu.SemaphoreType.DMA((N_DEV,)),
        ],
        compiler_params=pltpu.CompilerParams(collective_id=cid, has_side_effects=True),
        name=f'fetch_rows_{cid}',
    )(tok_req.reshape(N_DEV, TOK_SLOTS, 1), tok_place.reshape(seq, 1), table)


def give_body(dx_ref, tok_place_ref, pos_place_ref, tok_req_ref, pos_req_ref, vec_ref, tok_ref, pos_ref, vec_out_ref,
              send_buf, tok_buf, pos_buf, tok_acc, pos_acc, send_sem, recv_sem):
    me = lax.axis_index('fsdp')
    seq, model = dx_ref.shape
    both = TOK_SLOTS + POS_SLOTS
    enter_all(me)

    def remotes(off):
        peer = lax.rem(me + off, N_DEV)
        pairs = ((send_buf.at[off, pl.ds(0, TOK_SLOTS)], tok_buf.at[off]),
                 (send_buf.at[off, pl.ds(TOK_SLOTS, POS_SLOTS)], pos_buf.at[off]),
                 (vec_ref.at[peer], vec_out_ref.at[off]))
        return [pltpu.make_async_remote_copy(
            src_ref=src, dst_ref=dst, send_sem=send_sem.at[k, off], recv_sem=recv_sem.at[k, off],
            device_id=(peer,), device_id_type=pl.DeviceIdType.MESH) for k, (src, dst) in enumerate(pairs)]

    row = iota((both, 1), 0)
    is_tok = row < TOK_SLOTS

    def collect(off):
        peer = lax.rem(me + off, N_DEV)
        target = jnp.where(is_tok, peer * TOK_SLOTS + row, peer * POS_SLOTS + row - TOK_SLOTS)
        pick = (jnp.where(is_tok, tok_place_ref[...], pos_place_ref[...]) == target).astype(F32).astype(BF)
        return nn_dot(pick, dx_ref[...]).astype(BF)

    def produce(off, carry):
        send_buf[off] = collect(off)

        @pl.when(off >= 2)
        def _():
            for copy in remotes(off - 1):
                copy.start()
        return carry

    lax.fori_loop(1, N_DEV, produce, 0)
    own = collect(0)
    tok_buf[0] = own[:TOK_SLOTS]
    pos_buf[0] = own[TOK_SLOTS:]
    vec_out_ref[0] = vec_ref[me]
    for copy in remotes(N_DEV - 1):
        copy.start()

    last = N_DEV // GROUP - 1
    for g in range(N_DEV // GROUP):
        for off in range(g * GROUP, (g + 1) * GROUP):
            if off:
                for copy in remotes(off):
                    copy.wait_recv()
        for slots, buf, req_ref, acc_ref, out_ref in (
                (TOK_SLOTS, tok_buf, tok_req_ref, tok_acc, tok_ref), (POS_SLOTS, pos_buf, pos_req_ref, pos_acc, pos_ref)):
            block = buf[pl.ds(g * GROUP, GROUP)].reshape(GROUP * slots, model)
            wanted = req_ref[g]

            def add_up(r, carry):
                span = pl.ds(r * TILE, TILE)
                pick = (iota((TILE, 1), 0) + r * TILE == wanted).astype(F32).astype(BF)
                add = nn_dot(pick, block)
                if g == 0:
                    acc_ref[span, :] = add
                elif g < last:
                    acc_ref[span, :] += add
                else:
                    out_ref[span, :] = (acc_ref[span, :] + add).astype(out_ref.dtype)
                return carry

            lax.fori_loop(0, acc_ref.shape[0] // TILE, add_up, 0)
    for off in range(1, N_DEV):
        for copy in remotes(off):
            copy.wait_send()


def give_rows(d_rows, tok_place, pos_place, tok_req, pos_req, vec, tok_rows, pos_rows, dtype, cid):
    seq, model = d_rows.shape
    source = lax.rem(lax.axis_index('fsdp') + N_DEV - jnp.arange(N_DEV), N_DEV)
    tok_req = jnp.take(tok_req, source, axis=0).reshape(N_DEV // GROUP, 1, GROUP * TOK_SLOTS)
    pos_req = jnp.take(pos_req, source, axis=0).reshape(N_DEV // GROUP, 1, GROUP * POS_SLOTS)
    return pl.pallas_call(
        give_body,
        out_shape=[
            jax.ShapeDtypeStruct((tok_rows, model), dtype),
            jax.ShapeDtypeStruct((pos_rows, model), dtype),
            jax.ShapeDtypeStruct(vec.shape, vec.dtype),
        ],
        in_specs=[pl.BlockSpec(memory_space=pltpu.VMEM)] * 6,
        out_specs=[pl.BlockSpec(memory_space=pltpu.VMEM)] * 3,
        scratch_shapes=[
            pltpu.VMEM((N_DEV, TOK_SLOTS + POS_SLOTS, model), BF),
            pltpu.VMEM((N_DEV, TOK_SLOTS, model), BF),
            pltpu.VMEM((N_DEV, POS_SLOTS, model), BF),
            pltpu.VMEM((tok_rows, model), F32),
            pltpu.VMEM((pos_rows, model), F32),
            pltpu.SemaphoreType.DMA((3, N_DEV)),
            pltpu.SemaphoreType.DMA((3, N_DEV)),
        ],
        compiler_params=pltpu.CompilerParams(collective_id=cid, has_side_effects=True),
        name=f'give_rows_{cid}',
    )(d_rows, tok_place.reshape(1, seq), pos_place.reshape(1, seq), tok_req, pos_req, vec)


def nt_dot(a, b):
    return lax.dot_general(a, b, (((1,), (1,)), ((), ())), preferred_element_type=F32)


def nn_dot(a, b):
    return lax.dot_general(a, b, (((1,), (0,)), ((), ())), preferred_element_type=F32)


def attn_fwd_tile(qi, q_ref, kv_ref, c_ref, lse_ref, s_ref, p_ref):
    q = q_ref[...] * BF(0.125)
    causal = lax.broadcasted_iota(jnp.int32, (TILE, TILE), 0) >= lax.broadcasted_iota(jnp.int32, (TILE, TILE), 1)
    lse = []
    for head in range(2):
        run_max = None
        for j in range(qi + 1):
            s = nt_dot(q, kv_ref[pl.ds(j * TILE, TILE), pl.ds(head * 128, 128)])
            if j == qi:
                s = jnp.where(causal, s, -1e30)
            s_ref[head, :, pl.ds(j * TILE, TILE)] = s
            part = jnp.maximum(s[:, :128], s[:, 128:])
            run_max = part if run_max is None else jnp.maximum(run_max, part)
        row_max = jnp.max(run_max, axis=1, keepdims=True)
        run_sum = None
        for j in range(qi + 1):
            e = jnp.exp(s_ref[head, :, pl.ds(j * TILE, TILE)] - row_max)
            s_ref[head, :, pl.ds(j * TILE, TILE)] = e
            part = e[:, :128] + e[:, 128:]
            run_sum = part if run_sum is None else run_sum + part
        row_sum = jnp.sum(run_sum, axis=1, keepdims=True)
        inv = 1.0 / row_sum
        for j in range(qi + 1):
            p_ref[head, :, pl.ds(j * TILE, TILE)] = (s_ref[head, :, pl.ds(j * TILE, TILE)] * inv).astype(BF)
        lse.append(row_max + jnp.log(row_sum))
    width = (qi + 1) * TILE
    c = nn_dot(p_ref[0, :, pl.ds(0, width)], kv_ref[pl.ds(0, width), pl.ds(256, 128)])
    c += nn_dot(p_ref[1, :, pl.ds(0, width)], kv_ref[pl.ds(0, width), pl.ds(384, 128)])
    c_ref[...] = c.astype(BF)
    lane = lax.broadcasted_iota(jnp.int32, (TILE, 128), 1)
    both = jnp.where(lane == 0, lse[0], lse[1])
    lse_ref[...] = both.T[:8, :]


def attn_fwd(qkv, kv4):
    seq = qkv.shape[0]
    model = qkv.shape[1] - 2 * HEAD
    pairs, blocks = model // 128, seq // TILE

    def body(*refs):
        for qi in range(blocks):
            @pl.when(pl.program_id(1) == qi)
            def _():
                attn_fwd_tile(qi, *refs)

    return pl.pallas_call(
        body,
        grid=(pairs, blocks),
        in_specs=[
            pl.BlockSpec((TILE, 128), lambda h, i: (i, h)),
            pl.BlockSpec((seq, 512), lambda h, i: (0, 0)),
        ],
        out_specs=[
            pl.BlockSpec((TILE, 128), lambda h, i: (i, h)),
            pl.BlockSpec((8, TILE), lambda h, i: (h, i)),
        ],
        out_shape=[
            jax.ShapeDtypeStruct((seq, model), BF),
            jax.ShapeDtypeStruct((8 * pairs, seq), F32),
        ],
        scratch_shapes=[pltpu.VMEM((2, TILE, seq), F32), pltpu.VMEM((2, TILE, seq), BF)],
        compiler_params=pltpu.CompilerParams(dimension_semantics=('arbitrary', 'arbitrary')),
        cost_estimate=pl.CostEstimate(flops=16 * seq * seq * model // 2, bytes_accessed=8 * seq * model, transcendentals=6 * seq * seq),
        name='attn_fwd',
    )(qkv, kv4)


def attn_bwd_tile(qi, q_ref, dc_ref, lse_ref, kv_ref, kt_ref, dq_ref, p_ref, pb_ref, dp_ref, ds_ref, q2_ref, dc2_ref, dk_acc, dv_acc):
    q = q_ref[...] * BF(0.125)
    dc = dc_ref[...]
    first = (lax.broadcasted_iota(jnp.int32, (1, 128), 1) < HEAD).astype(F32)
    for head in range(2):
        keep = (first if head == 0 else 1.0 - first).astype(BF)
        q2_ref[pl.ds(head * TILE, TILE), :] = q * keep
        dc2_ref[pl.ds(head * TILE, TILE), :] = dc * keep
    causal = lax.broadcasted_iota(jnp.int32, (TILE, TILE), 0) <= lax.broadcasted_iota(jnp.int32, (TILE, TILE), 1)
    width = (qi + 1) * TILE
    dq_parts = []
    for head in range(2):
        cols = pl.ds(head * TILE, TILE)
        lse_row = lse_ref[pl.ds(head, 1), :]
        run = None
        for j in range(qi + 1):
            rows = pl.ds(j * TILE, TILE)
            s = nt_dot(kv_ref[rows, pl.ds(head * 128, 128)], q)
            if j == qi:
                s = jnp.where(causal, s, -1e30)
            p = jnp.exp(s - lse_row)
            p_ref[rows, cols] = p
            pb_ref[rows, cols] = p.astype(BF)
            dp = nt_dot(kv_ref[rows, pl.ds(256 + head * 128, 128)], dc).astype(BF)
            dp_ref[rows, cols] = dp
            part = jnp.sum(p * dp.astype(F32), axis=0, keepdims=True)
            run = part if run is None else run + part
        for j in range(qi + 1):
            rows = pl.ds(j * TILE, TILE)
            ds_ref[rows, cols] = (p_ref[rows, cols] * (dp_ref[rows, cols].astype(F32) - run)).astype(BF)
        dq_parts.append(nn_dot(kt_ref[:, pl.ds(0, width)], ds_ref[pl.ds(0, width), cols]))
    dq_ref[...] = jnp.concatenate(dq_parts, axis=0).T.astype(BF)
    span = pl.ds(0, width)
    dv_acc[span, :] += nn_dot(pb_ref[span, :], dc2_ref[...])
    dk_acc[span, :] += nn_dot(ds_ref[span, :], q2_ref[...])


def attn_bwd(qkv, d_context, lse, kv4, k_t):
    seq = qkv.shape[0]
    model = qkv.shape[1] - 2 * HEAD
    pairs, blocks = model // 128, seq // TILE

    def body(q_ref, dc_ref, lse_ref, kv_ref, kt_ref, dq_ref, dkv_ref, *scratch):
        dk_acc, dv_acc = scratch[-2:]
        pair, block = pl.program_id(0), pl.program_id(1)

        @pl.when((pair == 0) & (block == 0))
        def _():
            dk_acc[...] = jnp.zeros_like(dk_acc)
            dv_acc[...] = jnp.zeros_like(dv_acc)

        for qi in range(blocks):
            @pl.when(block == qi)
            def _():
                attn_bwd_tile(qi, q_ref, dc_ref, lse_ref, kv_ref, kt_ref, dq_ref, *scratch)

        @pl.when((pair == pairs - 1) & (block == blocks - 1))
        def _():
            dk = dk_acc[...]
            dv = dv_acc[...]
            lane = lax.broadcasted_iota(jnp.int32, dk.shape, 1)
            both = jnp.where(lane < HEAD, dk + pltpu.roll(dk, HEAD, 1), dv + pltpu.roll(dv, HEAD, 1))
            dkv_ref[...] = both.astype(BF)

    return pl.pallas_call(
        body,
        grid=(pairs, blocks),
        in_specs=[
            pl.BlockSpec((TILE, 128), lambda h, i: (i, h)),
            pl.BlockSpec((TILE, 128), lambda h, i: (i, h)),
            pl.BlockSpec((8, TILE), lambda h, i: (h, i)),
            pl.BlockSpec((seq, 512), lambda h, i: (0, 0)),
            pl.BlockSpec((HEAD, seq), lambda h, i: (0, 0)),
        ],
        out_specs=[
            pl.BlockSpec((TILE, 128), lambda h, i: (i, h)),
            pl.BlockSpec((seq, 128), lambda h, i: (0, 0)),
        ],
        out_shape=[
            jax.ShapeDtypeStruct((seq, model), BF),
            jax.ShapeDtypeStruct((seq, 128), BF),
        ],
        scratch_shapes=[
            pltpu.VMEM((seq, 2 * TILE), F32),
            pltpu.VMEM((seq, 2 * TILE), BF),
            pltpu.VMEM((seq, 2 * TILE), BF),
            pltpu.VMEM((seq, 2 * TILE), BF),
            pltpu.VMEM((2 * TILE, 128), BF),
            pltpu.VMEM((2 * TILE, 128), BF),
            pltpu.VMEM((seq, 128), F32),
            pltpu.VMEM((seq, 128), F32),
        ],
        compiler_params=pltpu.CompilerParams(dimension_semantics=('arbitrary', 'arbitrary')),
        cost_estimate=pl.CostEstimate(flops=40 * seq * seq * model // 2, bytes_accessed=10 * seq * model, transcendentals=6 * seq * seq),
        name='attn_bwd',
    )(qkv, d_context, lse, kv4, k_t)


def layer_norm(rows_in, ln_gain, ln_shift):
    row_mean = jnp.mean(rows_in, axis=-1, keepdims=True)
    centered = rows_in - row_mean
    row_var = jnp.mean(centered * centered, axis=-1, keepdims=True)
    return centered * lax.rsqrt(row_var + 1e-5) * ln_gain + ln_shift


def gelu_tanh(pre_act):
    return jax.nn.gelu(pre_act, approximate=True)


def row_major(a):
    return with_layout_constraint(a, Layout(major_to_minor=tuple(range(a.ndim))))


def tn_dot(a, b):
    return lax.dot_general(a, b, (((0,), (0,)), ((), ())), preferred_element_type=F32)


def scatter_sum(grad):
    return lax.psum_scatter(grad, 'fsdp', scatter_dimension=0, tiled=True)


def layer_pass(x_emb, grad_out, weights):
    (ln1_gain, ln1_bias, w_qkv, b_qkv, w_out, b_out, ln2_gain, ln2_bias, w_fc, b_fc, w_proj, b_proj) = weights
    model = x_emb.shape[1]
    x_res = x_emb.astype(F32)
    ln1_out, pull_ln1 = jax.vjp(layer_norm, x_res, ln1_gain, ln1_bias)
    ln1_act = ln1_out.astype(BF)
    qkv = row_major((nn_dot(ln1_act, w_qkv) + b_qkv).astype(BF))
    key, value = qkv[:, model:model + HEAD], qkv[:, model + HEAD:]
    zero = jnp.zeros_like(key)
    kv4 = jnp.concatenate([key, zero, zero, key, value, zero, zero, value], axis=1)
    k_t = (key * BF(0.125)).T
    context, lse = attn_fwd(qkv, kv4)
    hidden1 = (x_res + nn_dot(context, w_out) + b_out).astype(BF)
    h1_wide = hidden1.astype(F32)
    ln2_out, pull_ln2 = jax.vjp(layer_norm, h1_wide, ln2_gain, ln2_bias)
    ln2_act = ln2_out.astype(BF)
    pre_fc = (nn_dot(ln2_act, w_fc) + b_fc).astype(BF)
    gelu_val, pull_gelu = jax.vjp(gelu_tanh, pre_fc.astype(F32))
    act_fc = gelu_val.astype(BF)
    hidden_out = (h1_wide + nn_dot(act_fc, w_proj) + b_proj).astype(BF)

    dy_wide = grad_out.astype(F32)
    g_b_proj = jnp.sum(dy_wide, axis=0)
    g_w_proj = tn_dot(act_fc, grad_out)
    d_act_fc = nt_dot(grad_out, w_proj).astype(BF)
    d_pre_fc = pull_gelu(d_act_fc.astype(F32))[0].astype(BF)
    g_b_fc = jnp.sum(d_pre_fc, axis=0, dtype=F32)
    g_w_fc = tn_dot(ln2_act, d_pre_fc)
    d_ln2_act = nt_dot(d_pre_fc, w_fc).astype(BF)
    d_h1_norm, g_ln2_gain, g_ln2_bias = pull_ln2(d_ln2_act.astype(F32))
    d_hidden1 = (dy_wide + d_h1_norm).astype(BF)
    g_b_out = jnp.sum(d_hidden1, axis=0, dtype=F32)
    g_w_out = tn_dot(context, d_hidden1)
    d_context = row_major(nt_dot(d_hidden1, w_out).astype(BF))
    g_w_proj = scatter_sum(g_w_proj)
    d_context, g_w_out, g_w_fc, g_w_proj = lax.optimization_barrier((d_context, g_w_out, g_w_fc, g_w_proj))
    g_w_fc, g_w_out = scatter_sum(g_w_fc), scatter_sum(g_w_out)
    d_query, d_kv = attn_bwd(qkv, d_context, lse, kv4, k_t)
    d_qkv = jnp.concatenate([d_query, d_kv], axis=1)
    g_b_qkv = jnp.sum(d_qkv, axis=0, dtype=F32)
    g_w_qkv = tn_dot(ln1_act, d_qkv)
    d_ln1_act = nt_dot(d_qkv, w_qkv).astype(BF)
    d_x_norm, g_ln1_gain, g_ln1_bias = pull_ln1(d_ln1_act.astype(F32))
    d_x0 = d_hidden1.astype(F32) + d_x_norm
    vec_grads = (g_ln1_gain, g_ln1_bias, g_b_qkv, g_b_out, g_ln2_gain, g_ln2_bias, g_b_fc, g_b_proj)
    mat_grads = (g_w_qkv, g_w_out, g_w_fc, g_w_proj)
    return hidden_out, d_x0, vec_grads, mat_grads


def slots_of(ids):
    stripe = lax.rem(ids, N_DEV)
    order = jnp.arange(ids.shape[0])
    earlier = (stripe[:, None] == stripe[None, :]) & (order[None, :] < order[:, None])
    return stripe, jnp.sum(earlier.astype(jnp.int32), axis=1)


def round_place(stripe, slot, per_peer, rnd):
    local = slot - rnd * per_peer
    return jnp.where((local >= 0) & (local < per_peer), stripe * per_peer + local, -1)


def requests(place, rows, per_peer):
    total = N_DEV * per_peer
    hit = jnp.arange(total)[:, None] == place[None, :]
    return jnp.max(jnp.where(hit, rows[None, :], -1), axis=1).reshape(N_DEV, per_peer)


def solution(mesh):
    vec_spec = P('fsdp')
    mat_spec = P('fsdp', None)
    act_spec = P('fsdp', None, None)
    param_specs = (vec_spec, vec_spec, mat_spec, vec_spec, mat_spec, vec_spec, vec_spec, vec_spec, mat_spec, vec_spec, mat_spec, vec_spec)
    in_specs = (mat_spec, mat_spec, mat_spec, mat_spec) + param_specs + (act_spec,)
    out_specs = (act_spec, mat_spec, mat_spec) + param_specs

    def device_body(tokens, positions, tok_table, pos_table, ln1_gain, ln1_bias, w_qkv, b_qkv, w_out, b_out, ln2_gain, ln2_bias, w_fc, b_fc, w_proj, b_proj, grad_out):
        tokens, positions, grad_out = tokens[0], positions[0], grad_out[0]
        tok_rows, model = tok_table.shape
        pos_rows = pos_table.shape[0]
        tok_sub, pos_sub = tok_rows // N_DEV, pos_rows // N_DEV

        pos_full = lax.all_gather(pos_table.astype(BF), 'fsdp', axis=0, tiled=True)
        qkv_full = lax.all_gather(w_qkv.astype(BF), 'fsdp', axis=0, tiled=True)

        tok_row = lax.div(tokens, tok_rows) * tok_sub + lax.div(lax.rem(tokens, tok_rows), N_DEV)
        pos_row = lax.div(positions, pos_rows) * pos_sub + lax.div(lax.rem(positions, pos_rows), N_DEV)
        tok_stripe, tok_slot = slots_of(tokens)
        pos_stripe, pos_slot = slots_of(positions)
        my_rounds = jnp.maximum(lax.div(jnp.max(tok_slot), TOK_SLOTS), lax.div(jnp.max(pos_slot), POS_SLOTS)) + 1

        def places(rnd):
            return round_place(tok_stripe, tok_slot, TOK_SLOTS, rnd), round_place(pos_stripe, pos_slot, POS_SLOTS, rnd)

        def request_block(tok_place, pos_place):
            tok_req = requests(tok_place, tok_row, TOK_SLOTS)
            pos_req = requests(pos_place, pos_row, POS_SLOTS)
            rounds = jnp.broadcast_to(my_rounds, (N_DEV, 1))
            flat = jnp.concatenate([tok_req, pos_req, rounds], axis=1)
            return jnp.pad(flat, ((0, 0), (0, 1024 - flat.shape[1]))).reshape(N_DEV, 8, 128)

        def read_block(block):
            flat = block.reshape(N_DEV, 1024)
            tok_req = flat[:, :TOK_SLOTS]
            pos_req = flat[:, TOK_SLOTS:TOK_SLOTS + POS_SLOTS]
            return tok_req, pos_req, jnp.max(flat[:, TOK_SLOTS + POS_SLOTS])

        def stripes(table, sub):
            return table.astype(BF).reshape(sub, N_DEV, model).transpose(1, 0, 2)

        shards = (ln1_gain, ln1_bias, b_qkv, b_out, ln2_gain, ln2_bias, b_fc, b_proj)
        sizes = [v.shape[0] for v in shards]
        vec_block = jnp.pad(jnp.concatenate(shards), (0, 1024 - sum(sizes))).reshape(8, 128)
        tok_place, pos_place = places(0)
        tok_stripes, req_in, vec_all = exchange([stripes(tok_table, tok_sub), request_block(tok_place, pos_place)], [vec_block], 0)
        tok_stripes = tok_stripes.reshape(tok_rows, model)
        vec_flat = vec_all.reshape(N_DEV, 1024).astype(BF).astype(F32)
        vecs, start = [], 0
        for size in sizes:
            vecs.append(vec_flat[:, start:start + size].reshape(-1))
            start += size

        tok_req0, pos_req0, rounds = read_block(req_in)
        def slow_fetch():
            def step(state):
                rnd, x_sum = state
                tok_place, pos_place = places(rnd)
                (block,) = exchange([request_block(tok_place, pos_place)], [], 2)
                return rnd + 1, x_sum + fetch_rows(read_block(block)[0], tok_place, tok_stripes, 3)

            _, x_sum = lax.while_loop(lambda state: state[0] < rounds, step, (jnp.int32(0), jnp.zeros((tokens.shape[0], model), BF)))
            return x_sum

        x_tok = fetch_rows(tok_req0, tok_place, tok_stripes, 1)
        x_tok = lax.cond(rounds > 1, slow_fetch, lambda: x_tok)
        x_pos = jnp.take(pos_full, positions, axis=0)
        x_emb = (x_tok.astype(F32) + x_pos.astype(F32)).astype(BF)
        x_emb, late = lax.optimization_barrier((x_emb, (w_out.astype(BF), w_fc.astype(BF), w_proj.astype(BF))))
        full = [qkv_full] + [lax.all_gather(w, 'fsdp', axis=0, tiled=True) for w in late]

        weights = (vecs[0], vecs[1], full[0], vecs[2], full[1], vecs[3], vecs[4], vecs[5], full[2], vecs[6], full[3], vecs[7])
        hidden_out, d_x0, vec_grads, mat_grads = layer_pass(x_emb, grad_out, weights)
        d_rows = d_x0.astype(BF)

        d_rows, g_qkv, early = lax.optimization_barrier((d_rows, mat_grads[0], mat_grads[1:]))
        g_mats = [scatter_sum(g_qkv)] + list(early)

        vec_out = jnp.concatenate([g.reshape(N_DEV, -1) for g in vec_grads], axis=1)
        vec_out = jnp.pad(vec_out, ((0, 0), (0, 1024 - vec_out.shape[1]))).reshape(N_DEV, 8, 128)

        tok_sum, pos_sum, vec_in = give_rows(d_rows, tok_place, pos_place, tok_req0, pos_req0, vec_out, tok_rows, pos_rows, BF, 4)

        def slow_give():
            def step(state):
                rnd, tok_sum, pos_sum = state
                tok_place, pos_place = places(rnd)
                (block,) = exchange([request_block(tok_place, pos_place)], [], 5)
                tok_req, pos_req, _ = read_block(block)
                tok_add, pos_add, _ = give_rows(d_rows, tok_place, pos_place, tok_req, pos_req, vec_out, tok_rows, pos_rows, F32, 7)
                return rnd + 1, tok_sum + tok_add, pos_sum + pos_add

            zeros = (jnp.zeros((tok_rows, model), F32), jnp.zeros((pos_rows, model), F32))
            _, tok_sum, pos_sum = lax.while_loop(lambda state: state[0] < rounds, step, (jnp.int32(0),) + zeros)
            return tok_sum.astype(BF), pos_sum.astype(BF)

        tok_sum, pos_sum = lax.cond(rounds > 1, slow_give, lambda: (tok_sum, pos_sum))
        tok_back, pos_back = exchange([tok_sum.reshape(N_DEV, tok_sub, model), pos_sum.reshape(N_DEV, pos_sub, model)], [], 6)
        g_tok = tok_back.transpose(1, 0, 2).reshape(tok_rows, model).astype(F32)
        g_pos = pos_back.transpose(1, 0, 2).reshape(pos_rows, model).astype(F32)

        vec_sum = jnp.sum(vec_in.reshape(N_DEV, 1024), axis=0)
        g_vecs, start = [], 0
        for size in sizes:
            g_vecs.append(vec_sum[start:start + size])
            start += size
        return (hidden_out[None], g_tok, g_pos, g_vecs[0], g_vecs[1], g_mats[0], g_vecs[2], g_mats[1], g_vecs[3],
                g_vecs[4], g_vecs[5], g_mats[2], g_vecs[6], g_mats[3], g_vecs[7])

    return jax.shard_map(device_body, mesh=mesh, in_specs=in_specs, out_specs=out_specs, check_vma=False)
```
